32 devices in a mesh: fsdp: 16 (over z, y, x), rep: 2 (over core).
Axes of the slice: x: 2, y: 2, z: 4, core: 2. Of those that a mesh axis runs over, the one named last changes fastest.
Arguments:
- params: float32 [1536, 3584], P(('fsdp', 'rep')), may hold values from -6 to 6
- grads: bfloat16 [1536, 3584], P(('fsdp', 'rep')), may hold values from -6 to 6
- moments: bfloat16 [3, 1536, 3584], P(None, ('fsdp', 'rep')), may hold values from -6 to 6
- row_acc: float32 [1536], P(('fsdp', 'rep')), may hold values from 0.05 to 1
- lengths: int32 [32], replicated, may hold values from 1 to 384, 1536 in all
- tensor_order: int32 [32], replicated, may hold values from 0 to 31, each once
- col_acc: float32 [32, 3584], P('fsdp'), may hold values from 0.05 to 1
- hidden_state: float32 [32, 512], P('fsdp'), may hold values from -1 to 1
- cell_state: float32 [32, 512], P('fsdp'), may hold values from -4 to 4
- lstm_in: bfloat16 [10, 2048], replicated, may hold values from -2 to 2
- lstm_rec: bfloat16 [512, 2048], replicated, may hold values from -0.25 to 0.25
- lstm_bias: float32 [2048], replicated, may hold values from -3 to 3
- hyper_first: bfloat16 [512, 256], replicated, may hold values from -0.25 to 0.25
- hyper_rest: bfloat16 [512, 128], replicated, may hold values from -0.25 to 0.25
Outputs:
- update: float32 [1536, 3584], P(('fsdp', 'rep'))
- row_new: float32 [1536], P(('fsdp', 'rep'))
- col_new: float32 [32, 3584], P('fsdp')
- hidden_new: float32 [32, 512], P('fsdp')
- cell_new: float32 [32, 512], P('fsdp')
The draws below stay inside these ranges and needn't reach their ends.
Inputs may be any that keep to these rules, and one draw needn't show every extreme that they name: `lengths`: they sum to 1536; the largest is 384. `tensor_order`: owner slot i belongs to fsdp index i // 2; each tensor appears once.
All inputs are finite; a program needn't handle non-finite values.
Results may differ from the reference program's by a relative error of at most 0.019.
Values may be sent and summed in bfloat16 or wider, within the bound.
A program may use at most 64 MiB of HBM per device.

```python
import math
import jax
import jax.numpy as jnp
import numpy as np
from jax import lax

C = 3584
HID = 512
FIN = 8
HM = 32
OUT = 3
FT = 10
NT = 32
ROWS = 1536
MOST = 384


def column_levels(key):
    exponent = jax.random.uniform(jax.random.fold_in(key, 71), (C,), jnp.float32, -1.5, 1.5)
    return jnp.exp(exponent)


def draw_grads(key, part):
    levels = column_levels(key)
    draw_key = jax.random.fold_in(key, 101)
    random_part = jax.random.normal(draw_key, (ROWS, C), jnp.float32)
    return jnp.clip(random_part * levels[None, :], -6.0, 6.0).astype(jnp.bfloat16)


def draw_col_acc(key, part):
    levels = column_levels(key)
    slot_exponent = jax.random.uniform(jax.random.fold_in(key, 201), (NT, 1), jnp.float32, jnp.log(0.1), jnp.log(0.4))
    jitter_key = jax.random.fold_in(key, 203)
    jitter = 0.3 * jax.random.normal(jitter_key, (NT, C), jnp.float32)
    values = jnp.exp(slot_exponent + jitter) * (levels * levels)[None, :]
    return jnp.clip(values, 0.05, 1.0).astype(jnp.float32)


def block_levels(key, shape, cuts, smallest, largest):
    level = 1.0
    for axis_at, blocks in cuts:
        steps = jax.random.uniform(jax.random.fold_in(jax.random.fold_in(key, 6), axis_at), (blocks,), jnp.float32, smallest / len(cuts), largest / len(cuts))
        level = level * jnp.repeat(jnp.exp(steps), shape[axis_at] // blocks).reshape((-1,) + (1,) * (len(shape) - 1 - axis_at))
    return level


def split_up(number_of, total, reach, slope):
    portions = [(1 << 20) // math.isqrt(grade ** slope) + 1 for grade in range(2, number_of + 1)]
    rest, holding = total - reach - (number_of - 1), [1] * (number_of - 1)
    while rest > 0:
        candidates = [i for i in range(number_of - 1) if holding[i] < reach]
        mass, budget = sum([portions[i] for i in candidates]), rest
        for i in candidates:
            more = min(reach - holding[i], max(1, budget * portions[i] // mass), rest)
            holding[i] = holding[i] + more
            rest = rest - more
    return np.array([reach] + holding)


def uneven(stream_key, number_of, total, bound, slope):
    if number_of == 2:
        one = jax.random.randint(stream_key, (), max(1, total - bound), min(bound, total - 1) + 1)
        return jnp.stack([one, total - one])
    tallies = jnp.asarray(split_up(number_of, total, bound, slope), jnp.int32)
    pairs = (number_of - 1) // 2
    donor, sink = tallies[1:1 + 2 * pairs:2], tallies[2:2 + 2 * pairs:2]
    slack = jnp.minimum(donor - 1, bound - sink)
    shifted = jax.random.randint(jax.random.fold_in(stream_key, 1), (pairs,), 0, 1 << 20) % (slack + 1)
    tallies = tallies.at[1:1 + 2 * pairs:2].set(donor - shifted).at[2:2 + 2 * pairs:2].set(sink + shifted)
    return tallies[jax.random.permutation(jax.random.fold_in(stream_key, 2), number_of)]


def centred(stream_key, shape, width, most, split=(), held_as=jnp.bfloat16):
    result = width * jax.random.normal(stream_key, shape, jnp.float32)
    if split:
        result = result * block_levels(stream_key, shape, split, -0.22, 0.18)
    return jnp.clip(result, -most, most).astype(held_as)


def setup_inputs(seed: int = 0) -> dict:
    key_list = jax.random.split(jax.random.key(seed), 15)
    params = centred(key_list[0], (ROWS, C), 1.0, 6.0, ((0, 32),), jnp.float32)
    grads = draw_grads(jax.random.fold_in(key_list[14], 71), 0)
    moments = centred(key_list[2], (3, ROWS, C), 1.0, 6.0, ((1, 32),))
    row_acc = jnp.clip(jnp.exp(math.log(1.0) - 2.9957323 * jax.random.uniform(key_list[3], (ROWS,), jnp.float32) ** block_levels(key_list[3], (ROWS,), ((0, 32),), -0.2, 0.2)), 0.05, 1.0)
    lengths = uneven(key_list[4], NT, ROWS, MOST, 2).astype(jnp.int32)
    tensor_order = jax.random.permutation(key_list[5], NT).astype(jnp.int32)
    col_acc = draw_col_acc(jax.random.fold_in(key_list[14], 71), 0)
    hidden_state = jnp.clip(jax.random.uniform(key_list[7], (NT, HID), jnp.float32, -1.0, 1.0) * block_levels(key_list[7], (NT, HID), ((0, 16),), -0.4, 0.0), -1.0, 1.0)
    cell_state = centred(key_list[8], (NT, HID), 1.0, 4.0, ((0, 16),), jnp.float32)
    lstm_in = centred(key_list[9], (FT, 4 * HID), FT ** -0.5, 2.0)
    lstm_rec = centred(key_list[10], (HID, 4 * HID), HID ** -0.5, 0.25)
    lstm_bias = centred(key_list[11], (4 * HID,), 0.5, 3.0, (), jnp.float32)
    hyper_first = centred(key_list[12], (HID, FIN * HM), HID ** -0.5, 0.25)
    hyper_rest = centred(key_list[13], (HID, HM * (1 + OUT)), HID ** -0.5, 0.25)
    return {"params": params, "grads": grads, "moments": moments, "row_acc": row_acc, "lengths": lengths, "tensor_order": tensor_order, "col_acc": col_acc, "hidden_state": hidden_state, "cell_state": cell_state, "lstm_in": lstm_in, "lstm_rec": lstm_rec, "lstm_bias": lstm_bias, "hyper_first": hyper_first, "hyper_rest": hyper_rest}


EPSILON = 1e-06
DECAY_RATE = 0.9

def owner_step(col_sums, tensor_stats, row_lengths, col_acc, hidden_state, cell_state, lstm_in, lstm_rec, lstm_bias, hyper_first, hyper_rest):
    col_width = col_acc.shape[1]
    col_new = DECAY_RATE * col_acc + (1.0 - DECAY_RATE) * col_sums / row_lengths[:, None]
    tensor_means = tensor_stats / (row_lengths * col_width)[:, None]
    log_means = jnp.log(tensor_means[:, :5] + EPSILON)
    corr_first = tensor_means[:, 5] / jnp.sqrt(tensor_means[:, 0] * tensor_means[:, 1] + EPSILON)
    corr_second = tensor_means[:, 6] / jnp.sqrt(tensor_means[:, 0] * tensor_means[:, 3] + EPSILON)
    corr_third = tensor_means[:, 7] / jnp.sqrt(tensor_means[:, 1] * tensor_means[:, 3] + EPSILON)
    col_mean = lax.optimization_barrier(jnp.mean(col_new, axis=1))
    col_square = lax.optimization_barrier(jnp.mean(col_new * col_new, axis=1))
    spread = jnp.log(col_square / (col_mean * col_mean))
    extra = jnp.stack([corr_first, corr_second, corr_third, jnp.log(col_mean + EPSILON), spread], axis=1)
    features = jnp.concatenate([log_means, extra], axis=1).astype(jnp.bfloat16)
    gate_sum = jnp.dot(features, lstm_in, preferred_element_type=jnp.float32)
    gate_sum = gate_sum + jnp.dot(hidden_state.astype(jnp.bfloat16), lstm_rec, preferred_element_type=jnp.float32) + lstm_bias
    hid_width = hidden_state.shape[1]
    gate_in = gate_sum[:, :hid_width]
    gate_forget = gate_sum[:, hid_width:2 * hid_width]
    gate_cand = gate_sum[:, 2 * hid_width:3 * hid_width]
    gate_out = gate_sum[:, 3 * hid_width:]
    cell_new = jax.nn.sigmoid(gate_forget) * cell_state + jax.nn.sigmoid(gate_in) * jnp.tanh(gate_cand)
    hidden_new = jax.nn.sigmoid(gate_out) * jnp.tanh(cell_new)
    hidden_bf = hidden_new.astype(jnp.bfloat16)
    gen_first = jnp.dot(hidden_bf, hyper_first, preferred_element_type=jnp.float32).astype(jnp.bfloat16)
    gen_rest = jnp.dot(hidden_bf, hyper_rest, preferred_element_type=jnp.float32).astype(jnp.bfloat16)
    tensor_scales = jnp.stack([jnp.sqrt(tensor_means[:, 0] + EPSILON), jnp.sqrt(tensor_means[:, 1] + EPSILON), jnp.sqrt(tensor_means[:, 4] + EPSILON), col_mean], axis=1)
    return (col_new, hidden_new, cell_new, gen_first, gen_rest, tensor_scales)

def param_block(param_rows, grad_rows, moment_rows, row_var, col_rows, first_rows, rest_rows, scale_rows):
    block_rows = param_rows.shape[0]
    grad_f = grad_rows.astype(jnp.float32)
    mom_f = moment_rows.astype(jnp.float32)
    v_factored = row_var[:, None] * col_rows / scale_rows[:, 3:4]
    inv_rms = lax.rsqrt(v_factored + EPSILON)
    grad_norm = grad_f * inv_rms
    mom_norm = mom_f[0] * inv_rms
    inputs = jnp.stack([grad_norm, mom_norm, mom_f[1] * inv_rms, mom_f[2] * inv_rms, grad_f / scale_rows[:, 0:1], mom_f[0] / scale_rows[:, 1:2], param_rows / scale_rows[:, 2:3], grad_norm * mom_norm], axis=1).astype(jnp.bfloat16)
    hm_width = rest_rows.shape[1] // 4
    w_first = first_rows.astype(jnp.float32).reshape(block_rows, 8, hm_width)
    bias_first = rest_rows[:, :hm_width].astype(jnp.float32)
    w_second = rest_rows[:, hm_width:].astype(jnp.float32).reshape(block_rows, hm_width, 3)
    hidden_units = jnp.einsum('bfc,bfh->bhc', inputs.astype(jnp.float32), w_first) + bias_first[:, :, None]
    hidden_units = jax.nn.relu(hidden_units).astype(jnp.bfloat16)
    mlp_out = jnp.einsum('bhc,bho->boc', hidden_units.astype(jnp.float32), w_second)
    return mlp_out[:, 0] * jnp.exp(jnp.tanh(mlp_out[:, 1])) * jax.nn.sigmoid(mlp_out[:, 2])

def reference(params, grads, moments, row_acc, lengths, tensor_order, col_acc, hidden_state, cell_state, lstm_in, lstm_rec, lstm_bias, hyper_first, hyper_rest):
    row_count = params.shape[0]
    tensor_count = lengths.shape[0]
    tensor_ends = jnp.cumsum(lengths).astype(jnp.int32)
    row_ids = jnp.arange(row_count, dtype=jnp.int32)
    seg_ids = lax.optimization_barrier(jnp.sum((row_ids[:, None] >= tensor_ends[None, :]).astype(jnp.int32), axis=1))
    grad_f = grads.astype(jnp.float32)
    grad_sq = grad_f * grad_f
    row_new = DECAY_RATE * row_acc + (1.0 - DECAY_RATE) * lax.optimization_barrier(jnp.mean(grad_sq, axis=1))
    mom_zero = moments[0].astype(jnp.float32)
    mom_one = moments[1].astype(jnp.float32)
    mom_two = moments[2].astype(jnp.float32)
    per_row = jnp.stack([lax.optimization_barrier(jnp.sum(grad_sq, axis=1)), lax.optimization_barrier(jnp.sum(mom_zero * mom_zero, axis=1)), lax.optimization_barrier(jnp.sum(mom_one * mom_one, axis=1)), lax.optimization_barrier(jnp.sum(mom_two * mom_two, axis=1)), lax.optimization_barrier(jnp.sum(params * params, axis=1)), lax.optimization_barrier(jnp.sum(grad_f * mom_zero, axis=1)), lax.optimization_barrier(jnp.sum(grad_f * mom_two, axis=1)), lax.optimization_barrier(jnp.sum(mom_zero * mom_two, axis=1))], axis=1)
    tensor_stats = jax.ops.segment_sum(per_row, seg_ids, num_segments=tensor_count)
    col_sums = jax.ops.segment_sum(grad_sq, seg_ids, num_segments=tensor_count)
    row_lengths = lengths[tensor_order].astype(jnp.float32)
    col_new, hidden_new, cell_new, gen_first, gen_rest, tensor_scales = owner_step(col_sums[tensor_order], tensor_stats[tensor_order], row_lengths, col_acc, hidden_state, cell_state, lstm_in, lstm_rec, lstm_bias, hyper_first, hyper_rest)
    col_table = jnp.zeros_like(col_new).at[tensor_order].set(col_new)
    first_table = jnp.zeros_like(gen_first).at[tensor_order].set(gen_first)
    rest_table = jnp.zeros_like(gen_rest).at[tensor_order].set(gen_rest)
    scale_table = jnp.zeros_like(tensor_scales).at[tensor_order].set(tensor_scales)
    block_rows = 64
    block_count = row_count // block_rows

    def one_block(index):
        start = (index * block_rows).astype(jnp.int32)
        seg_block = lax.dynamic_slice_in_dim(seg_ids, start, block_rows, 0)
        return param_block(lax.dynamic_slice_in_dim(params, start, block_rows, 0), lax.dynamic_slice_in_dim(grads, start, block_rows, 0), lax.dynamic_slice_in_dim(moments, start, block_rows, 1), lax.dynamic_slice_in_dim(row_new, start, block_rows, 0), col_table[seg_block], first_table[seg_block], rest_table[seg_block], scale_table[seg_block])
    update = lax.map(one_block, jnp.arange(block_count, dtype=jnp.int32)).reshape(params.shape)
    return (update, row_new, col_new, hidden_new, cell_new)
```

```python
import functools
import math

import jax
import jax.numpy as jnp
from jax import lax
from jax.experimental import pallas as pl
from jax.experimental.pallas import tpu as pltpu
from jax.sharding import PartitionSpec as P

EPSILON = 1e-06
DECAY_RATE = 0.9
LANES = 128
GROUP = 16
STATS = 8
F32 = jnp.float32
BF16 = jnp.bfloat16


def iota(shape, axis):
    return lax.broadcasted_iota(jnp.int32, shape, axis)


def to_column(row):
    size = row.shape[1]
    square = jnp.broadcast_to(row, (size, size))
    return jnp.sum(jnp.where(iota((size, size), 0) == iota((size, size), 1), square, 0.0), 1, keepdims=True)


def to_row(column):
    size = column.shape[0]
    square = jnp.broadcast_to(column, (size, size))
    return jnp.sum(jnp.where(iota((size, size), 0) == iota((size, size), 1), square, 0.0), 0, keepdims=True)


def take_rows(table, first, out):
    for j in range(out.shape[0]):
        mine = iota(table.shape, 0) == first + j
        out[j : j + 1, :] = jnp.sum(jnp.where(mine, table, 0.0), 0, keepdims=True)


def slot_columns(lengths, order):
    count = lengths.shape[1]
    order_col = to_column(order)
    tensor = iota((count, count), 1).astype(F32)
    spread = jnp.broadcast_to(lengths, (count, count))
    start = jnp.sum(jnp.where(tensor < order_col, spread, 0.0), 1, keepdims=True)
    size = jnp.sum(jnp.where(tensor == order_col, spread, 0.0), 1, keepdims=True)
    return start, size


def share_kernel(
    fsdp,
    rep,
    params_ref,
    grads_ref,
    moments_ref,
    lengths_ref,
    order_ref,
    col_acc_ref,
    hidden_ref,
    cell_ref,
    cols_out,
    hidden_out,
    cell_out,
    rows_out,
    part,
    held,
    total,
    cols,
    acc_parts,
    acc_all,
    hidden_parts,
    cell_parts,
    sems,
    send_sem,
    acc_sem,
):
    count = fsdp * rep
    my_f = lax.axis_index("fsdp")
    my_r = lax.axis_index("rep")
    me = my_f * rep + my_r
    row_count, width = params_ref.shape
    slots = lengths_ref.shape[1]
    own = slots // fsdp
    tiles = width // LANES
    all_tiles = tiles + 1
    barrier = pltpu.get_barrier_semaphore()

    def hello(k, _):
        to = lax.rem(me + k, count)
        pl.semaphore_signal(
            barrier,
            inc=1,
            device_id=(to // rep, lax.rem(to, rep)),
            device_id_type=pl.DeviceIdType.MESH,
        )
        return 0

    lax.fori_loop(1, count, hello, 0)

    start, size = slot_columns(lengths_ref[...].astype(F32), order_ref[...].astype(F32))
    row_ids = (me * row_count + iota((slots, row_count), 1)).astype(F32)
    pick = jnp.where((row_ids >= start) & (row_ids < start + size), 1.0, 0.0)

    step = LANES * math.gcd(tiles, 4)
    lane = iota((GROUP, LANES), 1)
    for first in range(0, row_count, GROUP):
        rows = pl.ds(first, GROUP)

        def chunk(k, sums):
            at = pl.ds(pl.multiple_of(k * step, LANES), step)
            g = grads_ref[rows, at].astype(F32)
            m0 = moments_ref[0, rows, at].astype(F32)
            m1 = moments_ref[1, rows, at].astype(F32)
            m2 = moments_ref[2, rows, at].astype(F32)
            p = params_ref[rows, at]
            pairs = ((g, g), (m0, m0), (m1, m1), (m2, m2), (p, p), (g, m0), (g, m2), (m0, m2))
            new = []
            for s, (a, b) in zip(sums, pairs):
                prod = a * b
                for j in range(0, step, LANES):
                    s = s + prod[:, j : j + LANES]
                new.append(s)
            return tuple(new)

        zero = jnp.zeros((GROUP, LANES), F32)
        sums = lax.fori_loop(0, width // step, chunk, (zero,) * STATS)
        row_stats = zero
        for k, s in enumerate(sums):
            row_stats = jnp.where(lax.rem(lane, STATS) == k, jnp.sum(s, 1, keepdims=True), row_stats)
        rows_out[rows, :] = row_stats

    slot_stats = jnp.dot(
        pick, rows_out[...], precision=lax.Precision.HIGHEST, preferred_element_type=F32
    )
    wide_lane = iota((slots, LANES), 1)
    high = slot_stats.astype(BF16).astype(F32)
    part[:, width:] = jnp.where(wide_lane < STATS, high, slot_stats - high).astype(BF16)
    pick_bf = pick.astype(BF16)
    for first in range(0, width, step):
        g = grads_ref[:, first : first + step].astype(F32)
        part[:, first : first + step] = jnp.dot(
            pick_bf, (g * g).astype(BF16), preferred_element_type=F32
        ).astype(BF16)

    pl.semaphore_wait(barrier, count - 1)

    def await_bytes(ref, sem):
        pltpu.make_async_copy(ref, ref, sem).wait()

    def copy(src, dst, which, to_f, to_r, sending=None):
        return pltpu.make_async_remote_copy(
            src_ref=src,
            dst_ref=dst,
            send_sem=send_sem.at[which] if sending is None else sending,
            recv_sem=sems.at[which],
            device_id=(to_f, to_r),
            device_id_type=pl.DeviceIdType.MESH,
        )

    my_tile = pl.ds(pl.multiple_of(jnp.minimum(me, all_tiles - 1) * LANES, LANES), LANES)

    def part_copy(tile):
        return copy(
            part.at[:, pl.ds(tile * LANES, LANES)], held.at[me], 0, tile // rep, tile % rep
        )

    for tile in range(all_tiles):
        pl.when(me != tile)(lambda tile=tile: part_copy(tile).start())

    def acc_copy(q):
        tile = q * rep + my_r
        at = pl.ds(pl.multiple_of(tile * LANES, LANES), LANES)
        return copy(col_acc_ref.at[:, at], acc_parts.at[my_f], 1, q, my_r, acc_sem.at[q])

    acc_steps = -(-tiles // rep)
    for q in range(acc_steps):
        pl.when((q != my_f) & (q * rep + my_r < tiles))(lambda q=q: acc_copy(q).start())

    def state_copies(k):
        to = lax.rem(my_f + k, fsdp)
        return (
            copy(hidden_ref, hidden_parts.at[my_f], 2, to, my_r),
            copy(cell_ref, cell_parts.at[my_f], 3, to, my_r),
        )

    def send_states(k, _):
        for c in state_copies(k):
            c.start()
        return 0

    lax.fori_loop(1, fsdp, send_states, 0)
    hidden_parts[my_f] = hidden_ref[...]
    cell_parts[my_f] = cell_ref[...]

    def tile_sum():
        held[me] = part[:, my_tile]
        await_bytes(held.at[pl.ds(0, count - 1)], sems.at[0])

        def add(k, s):
            return s + held[k].astype(F32)

        return lax.fori_loop(0, count, add, jnp.zeros((slots, LANES), F32), unroll=4)

    @pl.when(me < tiles)
    def _():
        acc_parts[my_f] = col_acc_ref[:, my_tile]
        await_bytes(acc_parts.at[pl.ds(0, fsdp - 1)], sems.at[1])
        for f in range(fsdp):
            acc_all[f * own : (f + 1) * own, :] = acc_parts[f]
        new = DECAY_RATE * acc_all[...] + (1.0 - DECAY_RATE) * tile_sum() / size
        total[...] = new.astype(BF16)

    @pl.when(me == tiles)
    def _():
        s = tile_sum()
        both = jnp.where(
            wide_lane < STATS, s + pltpu.roll(s, LANES - STATS, 1), s + pltpu.roll(s, STATS, 1)
        )
        top = both.astype(BF16).astype(F32)
        total[...] = jnp.where(wide_lane < STATS, top, both - top).astype(BF16)

    def total_copy(k):
        to = lax.rem(me + k, count)
        return copy(total, cols.at[:, my_tile], 4, to // rep, lax.rem(to, rep))

    @pl.when(me < all_tiles)
    def _():
        def send(k, _):
            total_copy(k).start()
            return 0

        lax.fori_loop(1, count, send, 0)
        cols[:, my_tile] = total[...]

    await_bytes(hidden_parts.at[pl.ds(0, fsdp - 1)], sems.at[2])
    await_bytes(cell_parts.at[pl.ds(0, fsdp - 1)], sems.at[3])
    for f in range(fsdp):
        hidden_out[f * own : (f + 1) * own, :] = hidden_parts[f]
        cell_out[f * own : (f + 1) * own, :] = cell_parts[f]

    def await_tiles(number):
        await_bytes(cols.at[:, pl.ds(0, number * LANES)], sems.at[4])
        await_bytes(part.at[:, pl.ds(0, number * LANES)], send_sem.at[0])

    pl.when(me < all_tiles)(lambda: await_tiles(all_tiles - 1))
    pl.when(me >= all_tiles)(lambda: await_tiles(all_tiles))
    cols_out[...] = cols[...]

    for q in range(acc_steps):
        pl.when((q != my_f) & (q * rep + my_r < tiles))(lambda q=q: acc_copy(q).wait_send())
    await_bytes(hidden_parts.at[pl.ds(0, fsdp - 1)], send_sem.at[2])
    await_bytes(cell_parts.at[pl.ds(0, fsdp - 1)], send_sem.at[3])

    @pl.when(me < all_tiles)
    def _():
        await_bytes(held.at[pl.ds(0, count - 1)], send_sem.at[4])


def update_kernel(
    rep,
    own,
    params_ref,
    grads_ref,
    moments_ref,
    row_acc_ref,
    lengths_ref,
    order_ref,
    cols_ref,
    hidden_ref,
    cell_ref,
    rows_ref,
    lstm_in_ref,
    lstm_rec_ref,
    lstm_bias_ref,
    hyper_first_ref,
    hyper_rest_ref,
    update_ref,
    row_new_ref,
    col_new_ref,
    hidden_new_ref,
    cell_new_ref,
    cols_f32,
    w_first,
    w_second,
):
    my_f = lax.axis_index("fsdp")
    me = my_f * rep + lax.axis_index("rep")
    row_count, width = params_ref.shape
    slots, hid = hidden_ref.shape
    hm = hyper_rest_ref.shape[1] // 4
    fin = hyper_first_ref.shape[1] // hm
    outs = (hyper_rest_ref.shape[1] - hm) // hm
    mine = my_f * own

    lengths = lengths_ref[...].astype(F32)
    order = order_ref[...].astype(F32)
    start, size = slot_columns(lengths, order)

    cols_f32[...] = cols_ref[:, :width].astype(F32)
    take_rows(cols_f32[...], mine, col_new_ref)
    col_mean = jnp.mean(cols_f32[...], axis=1, keepdims=True)
    col_square = jnp.mean(cols_f32[...] * cols_f32[...], axis=1, keepdims=True)
    sent = cols_ref[:, width:].astype(F32)
    stats = (sent + pltpu.roll(sent, LANES - STATS, 1)) / (size * width)
    mean = [stats[:, k : k + 1] for k in range(STATS)]
    features = [jnp.log(mean[k] + EPSILON) for k in range(5)] + [
        mean[5] / jnp.sqrt(mean[0] * mean[1] + EPSILON),
        mean[6] / jnp.sqrt(mean[0] * mean[3] + EPSILON),
        mean[7] / jnp.sqrt(mean[1] * mean[3] + EPSILON),
        jnp.log(col_mean + EPSILON),
        jnp.log(col_square / (col_mean * col_mean)),
    ]
    ft = lstm_in_ref.shape[0]
    lane = iota((slots, ft), 1)
    feature_table = jnp.zeros((slots, ft), F32)
    for k, f in enumerate(features):
        feature_table = jnp.where(lane == k, f, feature_table)
    gates = (
        jnp.dot(feature_table.astype(BF16), lstm_in_ref[...], preferred_element_type=F32)
        + jnp.dot(hidden_ref[...].astype(BF16), lstm_rec_ref[...], preferred_element_type=F32)
        + lstm_bias_ref[...]
    )
    cell_new = jax.nn.sigmoid(gates[:, hid : 2 * hid]) * cell_ref[...] + jax.nn.sigmoid(
        gates[:, :hid]
    ) * jnp.tanh(gates[:, 2 * hid : 3 * hid])
    hidden_new = jax.nn.sigmoid(gates[:, 3 * hid :]) * jnp.tanh(cell_new)
    take_rows(hidden_new, mine, hidden_new_ref)
    take_rows(cell_new, mine, cell_new_ref)
    hidden_bf = hidden_new.astype(BF16)
    first_all = jnp.dot(hidden_bf, hyper_first_ref[...], preferred_element_type=F32).astype(BF16)
    rest_all = jnp.dot(hidden_bf, hyper_rest_ref[...], preferred_element_type=F32).astype(BF16)
    wide_lane = iota((slots, LANES), 1)
    scales = jnp.where(
        wide_lane == 0,
        lax.rsqrt(mean[0] + EPSILON),
        jnp.where(
            wide_lane == 1,
            lax.rsqrt(mean[1] + EPSILON),
            jnp.where(wide_lane == 2, lax.rsqrt(mean[4] + EPSILON), 1.0 / col_mean),
        ),
    )

    start_row, size_row = to_row(start), to_row(size)
    row_ids = (me * row_count + iota((row_count, slots), 0)).astype(F32)
    pick = jnp.where((row_ids >= start_row) & (row_ids < start_row + size_row), 1.0, 0.0)
    pick_bf = pick.astype(BF16)
    scale_rows = jnp.dot(
        pick, scales, precision=lax.Precision.HIGHEST, preferred_element_type=F32
    )
    row_new = DECAY_RATE * to_column(row_acc_ref[...]) + ((1.0 - DECAY_RATE) / width) * rows_ref[:, :1]
    row_new_ref[...] = to_row(row_new)
    row_coef = row_new * scale_rows[:, 3:4]

    fh = fin * hm
    swap = jnp.where(
        iota((fh, fh), 0) == lax.rem(iota((fh, fh), 1), fin) * hm + iota((fh, fh), 1) // fin, 1.0, 0.0
    ).astype(BF16)
    first_swapped = jnp.dot(first_all, swap, preferred_element_type=F32).astype(BF16)
    first_rows = jnp.dot(pick_bf, first_swapped, preferred_element_type=F32).astype(BF16)
    rest_rows = jnp.dot(pick_bf, rest_all, preferred_element_type=F32)
    rest_bf = rest_rows.astype(BF16)
    wide = fin * GROUP
    per = LANES // fin
    spread_shape = (LANES, per * wide)
    column = iota(spread_shape, 1)
    spread = jnp.where(
        iota(spread_shape, 0) == (column // wide) * fin + lax.rem(column, wide) // GROUP, 1.0, 0.0
    ).astype(BF16)
    first_wide = [
        jnp.dot(first_rows[:, j : j + LANES], spread, preferred_element_type=F32)
        for j in range(0, fh, LANES)
    ]
    on_diag = lax.rem(iota((GROUP, wide), 1), GROUP) == iota((GROUP, wide), 0)
    eye = iota((GROUP, GROUP), 0) == iota((GROUP, GROUP), 1)
    second_shape = (hyper_rest_ref.shape[1], hm * GROUP)
    on_second = lax.rem(iota((GROUP, hm * GROUP), 1), GROUP) == iota((GROUP, hm * GROUP), 0)
    groups = row_count // GROUP
    for h in range(hm):
        source = first_wide[h // per]
        at = (h % per) * wide
        for g in range(groups):
            rows = slice(g * GROUP, (g + 1) * GROUP)
            place = slice(h * GROUP, (h + 1) * GROUP)
            w_first[g, place, :wide] = jnp.where(
                on_diag, source[rows, at : at + wide], 0.0
            ).astype(BF16)
            w_first[g, place, wide:] = jnp.where(eye, rest_rows[rows, h : h + 1], 0.0).astype(BF16)
    for o in range(outs):
        pattern = jnp.where(
            iota(second_shape, 0) == hm + (iota(second_shape, 1) // GROUP) * outs + o, 1.0, 0.0
        ).astype(BF16)
        second = jnp.dot(rest_bf, pattern, preferred_element_type=F32)
        for g in range(groups):
            w_second[g, o * GROUP : (o + 1) * GROUP, :] = jnp.where(
                on_second, second[g * GROUP : (g + 1) * GROUP], 0.0
            ).astype(BF16)

    step = LANES * math.gcd(width // LANES, 2)
    ones = jnp.ones((GROUP, step), BF16)

    @pl.loop(0, width // step)
    def _(k):
        at = pl.ds(pl.multiple_of(k * step, LANES), step)
        col_rows = jnp.dot(pick_bf, cols_ref[:, at], preferred_element_type=F32)
        for g in range(groups):
            rows = slice(g * GROUP, (g + 1) * GROUP)
            inv = lax.rsqrt(col_rows[rows] * row_coef[rows] + EPSILON)
            grad = grads_ref[rows, at].astype(F32)
            mom = moments_ref[0, rows, at].astype(F32)
            grad_norm = grad * inv
            mom_norm = mom * inv
            parts = (
                grad_norm,
                mom_norm,
                moments_ref[1, rows, at].astype(F32) * inv,
                moments_ref[2, rows, at].astype(F32) * inv,
                grad * scale_rows[rows, 0:1],
                mom * scale_rows[rows, 1:2],
                params_ref[rows, at] * scale_rows[rows, 2:3],
                grad_norm * mom_norm,
            )
            inputs = jnp.concatenate([x.astype(BF16) for x in parts] + [ones], axis=0)
            units = jnp.dot(w_first[g], inputs, preferred_element_type=F32)
            units = jnp.maximum(units.astype(BF16), jnp.zeros((), BF16))
            result = jnp.dot(w_second[g], units, preferred_element_type=F32)
            update_ref[rows, at] = (
                result[:GROUP]
                * jnp.exp(jnp.tanh(result[GROUP : 2 * GROUP]))
                * jax.nn.sigmoid(result[2 * GROUP :])
            )


def on_device(
    fsdp,
    rep,
    params,
    grads,
    moments,
    row_acc,
    lengths,
    tensor_order,
    col_acc,
    hidden_state,
    cell_state,
    lstm_in,
    lstm_rec,
    lstm_bias,
    hyper_first,
    hyper_rest,
):
    count = fsdp * rep
    row_count, width = params.shape
    slots = lengths.shape[0]
    own, hid = hidden_state.shape
    hm = hyper_rest.shape[1] // 4
    fin = hyper_first.shape[1] // hm
    outs = (hyper_rest.shape[1] - hm) // hm
    groups = row_count // GROUP
    lengths = lengths.reshape(1, slots)
    order = tensor_order.reshape(1, slots)
    in_vmem = pl.BlockSpec(memory_space=pltpu.VMEM)

    cols, hidden_all, cell_all, row_stats = pl.pallas_call(
        functools.partial(share_kernel, fsdp, rep),
        out_shape=(
            jax.ShapeDtypeStruct((slots, width + LANES), BF16),
            jax.ShapeDtypeStruct((slots, hid), F32),
            jax.ShapeDtypeStruct((slots, hid), F32),
            jax.ShapeDtypeStruct((row_count, LANES), F32),
        ),
        in_specs=[in_vmem] * 8,
        out_specs=[in_vmem] * 4,
        scratch_shapes=[
            pltpu.VMEM((slots, width + LANES), BF16),
            pltpu.VMEM((count, slots, LANES), BF16),
            pltpu.VMEM((slots, LANES), BF16),
            pltpu.VMEM((slots, width + LANES), BF16),
            pltpu.VMEM((fsdp, own, LANES), F32),
            pltpu.VMEM((slots, LANES), F32),
            pltpu.VMEM((fsdp, own, hid), F32),
            pltpu.VMEM((fsdp, own, hid), F32),
            pltpu.SemaphoreType.DMA((5,)),
            pltpu.SemaphoreType.DMA((5,)),
            pltpu.SemaphoreType.DMA((-(-(width // LANES) // rep),)),
        ],
        compiler_params=pltpu.CompilerParams(collective_id=0, has_side_effects=True),
        name="share",
    )(params, grads, moments, lengths, order, col_acc, hidden_state, cell_state)

    update, row_new, col_new, hidden_new, cell_new = pl.pallas_call(
        functools.partial(update_kernel, rep, own),
        out_shape=(
            jax.ShapeDtypeStruct((row_count, width), F32),
            jax.ShapeDtypeStruct((1, row_count), F32),
            jax.ShapeDtypeStruct((own, width), F32),
            jax.ShapeDtypeStruct((own, hid), F32),
            jax.ShapeDtypeStruct((own, hid), F32),
        ),
        in_specs=[in_vmem] * 15,
        out_specs=[in_vmem] * 5,
        scratch_shapes=[
            pltpu.VMEM((slots, width), F32),
            pltpu.VMEM((groups, hm * GROUP, (fin + 1) * GROUP), BF16),
            pltpu.VMEM((groups, outs * GROUP, hm * GROUP), BF16),
        ],
        name="update",
    )(
        params,
        grads,
        moments,
        row_acc.reshape(1, row_count),
        lengths,
        order,
        cols,
        hidden_all,
        cell_all,
        row_stats,
        lstm_in,
        lstm_rec,
        lstm_bias.reshape(1, -1),
        hyper_first,
        hyper_rest,
    )
    return (update, row_new.reshape(row_count), col_new, hidden_new, cell_new)


def solution(mesh):
    rows = P(("fsdp", "rep"), None)
    flat = P(("fsdp", "rep"))
    own = P("fsdp", None)
    return jax.shard_map(
        functools.partial(on_device, mesh.shape["fsdp"], mesh.shape["rep"]),
        mesh=mesh,
        in_specs=(rows, rows, P(None, ("fsdp", "rep"), None), flat, P(), P(), own, own, own)
        + (P(),) * 5,
        out_specs=(rows, flat, own, own, own),
        check_vma=False,
    )
```

```python
import functools
import math

import jax
import jax.numpy as jnp
from jax import lax
from jax.experimental import pallas as pl
from jax.experimental.pallas import tpu as pltpu
from jax.sharding import PartitionSpec as P

EPSILON = 1e-06
DECAY_RATE = 0.9
LANES = 128
GROUP = 16
STATS = 8
F32 = jnp.float32
BF16 = jnp.bfloat16


def iota(shape, axis):
    return lax.broadcasted_iota(jnp.int32, shape, axis)


def to_column(row):
    size = row.shape[1]
    square = jnp.broadcast_to(row, (size, size))
    return jnp.sum(jnp.where(iota((size, size), 0) == iota((size, size), 1), square, 0.0), 1, keepdims=True)


def to_row(column):
    size = column.shape[0]
    square = jnp.broadcast_to(column, (size, size))
    return jnp.sum(jnp.where(iota((size, size), 0) == iota((size, size), 1), square, 0.0), 0, keepdims=True)


def take_rows(table, first, out):
    for j in range(out.shape[0]):
        mine = iota(table.shape, 0) == first + j
        out[j : j + 1, :] = jnp.sum(jnp.where(mine, table, 0.0), 0, keepdims=True)


def slot_columns(lengths, order):
    count = lengths.shape[1]
    order_col = to_column(order)
    tensor = iota((count, count), 1).astype(F32)
    spread = jnp.broadcast_to(lengths, (count, count))
    start = jnp.sum(jnp.where(tensor < order_col, spread, 0.0), 1, keepdims=True)
    size = jnp.sum(jnp.where(tensor == order_col, spread, 0.0), 1, keepdims=True)
    return start, size


def split_stats(sums, lane):
    both = jnp.where(
        lane < STATS, sums + pltpu.roll(sums, LANES - STATS, 1), sums + pltpu.roll(sums, STATS, 1)
    )
    top = both.astype(BF16).astype(F32)
    return jnp.where(lane < STATS, top, both - top).astype(BF16)


def share_kernel(
    fsdp,
    rep,
    params_hbm,
    grads_hbm,
    moments_hbm,
    rec_hbm,
    bias_ref,
    lengths_ref,
    order_ref,
    col_acc_ref,
    hidden_ref,
    cell_ref,
    cols_out,
    gates_out,
    cell_out,
    rows_out,
    params_ref,
    grads_ref,
    moments_ref,
    rec_ref,
    part,
    pair,
    mid,
    held,
    total,
    cols,
    acc_parts,
    acc_all,
    hidden_parts,
    hidden_all,
    cell_parts,
    load_sem,
    recv_sem,
    send_sem,
    acc_sem,
    mid_sem,
):
    count = fsdp * rep
    my_f = lax.axis_index("fsdp")
    my_r = lax.axis_index("rep")
    me = my_f * rep + my_r
    row_count, width = params_ref.shape
    slots = lengths_ref.shape[1]
    own = slots // fsdp
    tiles = width // LANES
    per_rep = -(-(tiles + 1) // rep)
    block = per_rep * LANES
    barrier = pltpu.get_barrier_semaphore()

    def hello(k, _):
        to = lax.rem(me + k, count)
        pl.semaphore_signal(
            barrier,
            inc=1,
            device_id=(to // rep, lax.rem(to, rep)),
            device_id_type=pl.DeviceIdType.MESH,
        )
        return 0

    lax.fori_loop(1, count, hello, 0)
    loads = [
        pltpu.make_async_copy(src, dst, load_sem.at[k])
        for k, (src, dst) in enumerate(
            (
                (grads_hbm, grads_ref),
                (moments_hbm, moments_ref),
                (params_hbm, params_ref),
                (rec_hbm, rec_ref),
            )
        )
    ]
    for c in loads:
        c.start()

    def await_bytes(ref, sem):
        pltpu.make_async_copy(ref, ref, sem).wait()

    def copy(src, dst, which, to_f, to_r, sending=None):
        return pltpu.make_async_remote_copy(
            src_ref=src,
            dst_ref=dst,
            send_sem=send_sem.at[which] if sending is None else sending,
            recv_sem=recv_sem.at[which],
            device_id=(to_f, to_r),
            device_id_type=pl.DeviceIdType.MESH,
        )

    start, size = slot_columns(lengths_ref[...].astype(F32), order_ref[...].astype(F32))
    row_ids = (me * row_count + iota((slots, row_count), 1)).astype(F32)
    pick = jnp.where((row_ids >= start) & (row_ids < start + size), 1.0, 0.0)

    pl.semaphore_wait(barrier, count - 1)

    def state_copies(k):
        to = lax.rem(my_f + k, fsdp)
        return (
            copy(hidden_ref, hidden_parts.at[my_f], 2, to, my_r),
            copy(cell_ref, cell_parts.at[my_f], 3, to, my_r),
        )

    def acc_copy(q):
        tile = jnp.minimum(my_r * per_rep + q, tiles - 1)
        at = pl.ds(pl.multiple_of(tile * LANES, LANES), LANES)
        return copy(col_acc_ref.at[:, at], acc_parts.at[my_f], 1, q, my_r, acc_sem.at[q])

    def sends_acc(q):
        return (q != my_f) & (my_r * per_rep + q < tiles)

    def send_states(k, _):
        for c in state_copies(k):
            c.start()
        return 0

    for q in range(per_rep):
        pl.when(sends_acc(q))(lambda q=q: acc_copy(q).start())
    lax.fori_loop(1, fsdp, send_states, 0)
    hidden_parts[my_f] = hidden_ref[...]
    cell_parts[my_f] = cell_ref[...]

    step = LANES * math.gcd(tiles, 4)
    for c in loads[:3]:
        c.wait()
    lane = iota((GROUP, LANES), 1)
    for first in range(0, row_count, GROUP):
        rows = pl.ds(first, GROUP)

        def chunk(k, sums):
            at = pl.ds(pl.multiple_of(k * step, LANES), step)
            g = grads_ref[rows, at].astype(F32)
            m0 = moments_ref[0, rows, at].astype(F32)
            m1 = moments_ref[1, rows, at].astype(F32)
            m2 = moments_ref[2, rows, at].astype(F32)
            p = params_ref[rows, at]
            pairs = ((g, g), (m0, m0), (m1, m1), (m2, m2), (p, p), (g, m0), (g, m2), (m0, m2))
            new = []
            for s, (a, b) in zip(sums, pairs):
                prod = a * b
                for j in range(0, step, LANES):
                    s = s + prod[:, j : j + LANES]
                new.append(s)
            return tuple(new)

        zero = jnp.zeros((GROUP, LANES), F32)
        sums = lax.fori_loop(0, width // step, chunk, (zero,) * STATS)
        row_stats = zero
        for k, s in enumerate(sums):
            row_stats = jnp.where(lax.rem(lane, STATS) == k, jnp.sum(s, 1, keepdims=True), row_stats)
        rows_out[rows, :] = row_stats

    slot_stats = jnp.dot(
        pick, rows_out[...], precision=lax.Precision.HIGHEST, preferred_element_type=F32
    )
    wide_lane = iota((slots, LANES), 1)
    high = slot_stats.astype(BF16).astype(F32)
    part[:, width : width + LANES] = jnp.where(wide_lane < STATS, high, slot_stats - high).astype(BF16)
    if rep * per_rep > tiles + 1:
        part[:, width + LANES :] = jnp.zeros((slots, rep * block - width - LANES), BF16)
    pick_bf = pick.astype(BF16)
    for first in range(0, width, step):
        g = grads_ref[:, first : first + step].astype(F32)
        part[:, first : first + step] = jnp.dot(
            pick_bf, (g * g).astype(BF16), preferred_element_type=F32
        ).astype(BF16)

    def block_of(r):
        return pl.ds(pl.multiple_of(r * block, LANES), block)

    def pair_copy(k):
        to = lax.rem(my_r + k, rep)
        return copy(part.at[:, block_of(to)], pair.at[my_r], 0, my_f, to)

    for k in range(1, rep):
        pair_copy(k).start()
    pair[my_r] = part[:, block_of(my_r)]
    await_bytes(pair.at[pl.ds(0, rep - 1)], recv_sem.at[0])
    stats_rep, stats_at = tiles // per_rep, tiles % per_rep
    for q in range(per_rep):
        at = slice(q * LANES, (q + 1) * LANES)
        s = pair[0, :, at].astype(F32)
        for r in range(1, rep):
            s = s + pair[r, :, at].astype(F32)
        value = s.astype(BF16)
        if q == stats_at:
            value = jnp.where(my_r == stats_rep, split_stats(s, wide_lane), value)
        mid[:, at] = value

    def mid_copy(q):
        return copy(
            mid.at[:, pl.ds(q * LANES, LANES)], held.at[my_f], 5, q, my_r, mid_sem.at[q]
        )

    for q in range(per_rep):
        pl.when(q != my_f)(lambda q=q: mid_copy(q).start())

    await_bytes(hidden_parts.at[pl.ds(0, fsdp - 1)], recv_sem.at[2])
    await_bytes(cell_parts.at[pl.ds(0, fsdp - 1)], recv_sem.at[3])
    for f in range(fsdp):
        hidden_all[f * own : (f + 1) * own, :] = hidden_parts[f]
        cell_out[f * own : (f + 1) * own, :] = cell_parts[f]
    loads[3].wait()
    gates_out[...] = (
        jnp.dot(hidden_all[...].astype(BF16), rec_ref[...], preferred_element_type=F32)
        + bias_ref[...]
    )

    holds = my_f < per_rep
    my_tile = my_r * per_rep + my_f
    at_tile = pl.ds(
        pl.multiple_of(jnp.minimum(my_tile, rep * per_rep - 1) * LANES, LANES), LANES
    )
    at_acc = pl.ds(pl.multiple_of(jnp.minimum(my_tile, tiles - 1) * LANES, LANES), LANES)
    at_mid = pl.ds(pl.multiple_of(jnp.minimum(my_f, per_rep - 1) * LANES, LANES), LANES)

    def tile_sum():
        held[my_f] = mid[:, at_mid]
        await_bytes(held.at[pl.ds(0, fsdp - 1)], recv_sem.at[5])
        s = held[0].astype(F32)
        for f in range(1, fsdp):
            s = s + held[f].astype(F32)
        return s

    @pl.when(holds & (my_tile < tiles))
    def _():
        acc_parts[my_f] = col_acc_ref[:, at_acc]
        await_bytes(acc_parts.at[pl.ds(0, fsdp - 1)], recv_sem.at[1])
        for f in range(fsdp):
            acc_all[f * own : (f + 1) * own, :] = acc_parts[f]
        new = DECAY_RATE * acc_all[...] + (1.0 - DECAY_RATE) * tile_sum() / size
        total[...] = new.astype(BF16)

    @pl.when(holds & (my_tile >= tiles))
    def _():
        total[...] = split_stats(tile_sum(), wide_lane)

    def total_copy(k):
        return copy(total, cols.at[:, at_tile], 4, lax.rem(my_f + k, fsdp), my_r)

    @pl.when(holds)
    def _():
        def send(k, _):
            total_copy(k).start()
            return 0

        lax.fori_loop(1, fsdp, send, 0)
        cols[:, at_tile] = total[...]

    def await_tiles(number):
        await_bytes(cols.at[:, pl.ds(0, number * LANES)], recv_sem.at[4])

    pl.when(holds)(lambda: await_tiles(per_rep - 1))
    pl.when(jnp.logical_not(holds))(lambda: await_tiles(per_rep))

    def block_copy(k):
        here = cols.at[:, block_of(my_r)]
        return copy(here, here, 6, my_f, lax.rem(my_r + k, rep))

    for k in range(1, rep):
        block_copy(k).start()
    await_bytes(cols.at[:, pl.ds(0, (rep - 1) * block)], recv_sem.at[6])
    cols_out[...] = cols[...]

    await_bytes(pair.at[pl.ds(0, rep - 1)], send_sem.at[0])
    for q in range(per_rep):
        pl.when(sends_acc(q))(lambda q=q: acc_copy(q).wait_send())
        pl.when(q != my_f)(lambda q=q: mid_copy(q).wait_send())
    await_bytes(hidden_parts.at[pl.ds(0, fsdp - 1)], send_sem.at[2])
    await_bytes(cell_parts.at[pl.ds(0, fsdp - 1)], send_sem.at[3])
    await_bytes(cols.at[:, pl.ds(0, (rep - 1) * block)], send_sem.at[6])

    @pl.when(holds)
    def _():
        await_bytes(held.at[pl.ds(0, fsdp - 1)], send_sem.at[4])


def update_kernel(
    rep,
    own,
    params_ref,
    grads_ref,
    moments_ref,
    row_acc_ref,
    lengths_ref,
    order_ref,
    cols_ref,
    gates_ref,
    cell_ref,
    rows_ref,
    lstm_in_ref,
    hyper_first_ref,
    hyper_rest_ref,
    update_ref,
    row_new_ref,
    col_new_ref,
    hidden_new_ref,
    cell_new_ref,
    cols_f32,
    w_first,
    w_second,
    bias,
):
    my_f = lax.axis_index("fsdp")
    me = my_f * rep + lax.axis_index("rep")
    row_count, width = params_ref.shape
    slots, hid = cell_ref.shape
    hm = hyper_rest_ref.shape[1] // 4
    fin = hyper_first_ref.shape[1] // hm
    outs = (hyper_rest_ref.shape[1] - hm) // hm
    mine = my_f * own

    lengths = lengths_ref[...].astype(F32)
    order = order_ref[...].astype(F32)
    start, size = slot_columns(lengths, order)

    cols_f32[...] = cols_ref[:, :width].astype(F32)
    take_rows(cols_f32[...], mine, col_new_ref)
    col_mean = jnp.mean(cols_f32[...], axis=1, keepdims=True)
    col_square = jnp.mean(cols_f32[...] * cols_f32[...], axis=1, keepdims=True)
    sent = cols_ref[:, width : width + LANES].astype(F32)
    stats = (sent + pltpu.roll(sent, LANES - STATS, 1)) / (size * width)
    mean = [stats[:, k : k + 1] for k in range(STATS)]
    features = [jnp.log(mean[k] + EPSILON) for k in range(5)] + [
        mean[5] / jnp.sqrt(mean[0] * mean[1] + EPSILON),
        mean[6] / jnp.sqrt(mean[0] * mean[3] + EPSILON),
        mean[7] / jnp.sqrt(mean[1] * mean[3] + EPSILON),
        jnp.log(col_mean + EPSILON),
        jnp.log(col_square / (col_mean * col_mean)),
    ]
    ft = lstm_in_ref.shape[0]
    lane = iota((slots, ft), 1)
    feature_table = jnp.zeros((slots, ft), F32)
    for k, f in enumerate(features):
        feature_table = jnp.where(lane == k, f, feature_table)
    gates = gates_ref[...] + jnp.dot(
        feature_table.astype(BF16), lstm_in_ref[...], preferred_element_type=F32
    )
    cell_new = jax.nn.sigmoid(gates[:, hid : 2 * hid]) * cell_ref[...] + jax.nn.sigmoid(
        gates[:, :hid]
    ) * jnp.tanh(gates[:, 2 * hid : 3 * hid])
    hidden_new = jax.nn.sigmoid(gates[:, 3 * hid :]) * jnp.tanh(cell_new)
    take_rows(hidden_new, mine, hidden_new_ref)
    take_rows(cell_new, mine, cell_new_ref)
    hidden_bf = hidden_new.astype(BF16)
    first_all = jnp.dot(hidden_bf, hyper_first_ref[...], preferred_element_type=F32).astype(BF16)
    rest_all = jnp.dot(hidden_bf, hyper_rest_ref[...], preferred_element_type=F32).astype(BF16)
    wide_lane = iota((slots, LANES), 1)
    scales = jnp.where(
        wide_lane == 0,
        lax.rsqrt(mean[0] + EPSILON),
        jnp.where(
            wide_lane == 1,
            lax.rsqrt(mean[1] + EPSILON),
            jnp.where(wide_lane == 2, lax.rsqrt(mean[4] + EPSILON), 1.0 / col_mean),
        ),
    )

    start_row, size_row = to_row(start), to_row(size)
    row_ids = (me * row_count + iota((row_count, slots), 0)).astype(F32)
    pick = jnp.where((row_ids >= start_row) & (row_ids < start_row + size_row), 1.0, 0.0)
    pick_bf = pick.astype(BF16)
    scale_rows = jnp.dot(
        pick, scales, precision=lax.Precision.HIGHEST, preferred_element_type=F32
    )
    row_new = DECAY_RATE * to_column(row_acc_ref[...]) + ((1.0 - DECAY_RATE) / width) * rows_ref[:, :1]
    row_new_ref[...] = to_row(row_new)
    row_coef = row_new * scale_rows[:, 3:4]

    fh = fin * hm
    swap = jnp.where(
        iota((fh, fh), 0) == lax.rem(iota((fh, fh), 1), fin) * hm + iota((fh, fh), 1) // fin, 1.0, 0.0
    ).astype(BF16)
    first_swapped = jnp.dot(first_all, swap, preferred_element_type=F32).astype(BF16)
    first_rows = jnp.dot(pick_bf, first_swapped, preferred_element_type=F32).astype(BF16)
    rest_rows = jnp.dot(pick_bf, rest_all, preferred_element_type=F32)
    rest_bf = rest_rows.astype(BF16)
    wide = fin * GROUP
    per = LANES // fin
    spread_shape = (LANES, per * wide)
    column = iota(spread_shape, 1)
    spread = jnp.where(
        iota(spread_shape, 0) == (column // wide) * fin + lax.rem(column, wide) // GROUP, 1.0, 0.0
    ).astype(BF16)
    first_wide = [
        jnp.dot(first_rows[:, j : j + LANES], spread, preferred_element_type=F32)
        for j in range(0, fh, LANES)
    ]
    on_diag = lax.rem(iota((GROUP, wide), 1), GROUP) == iota((GROUP, wide), 0)
    eye = iota((GROUP, GROUP), 0) == iota((GROUP, GROUP), 1)
    second_shape = (hyper_rest_ref.shape[1], hm * GROUP)
    on_second = lax.rem(iota((GROUP, hm * GROUP), 1), GROUP) == iota((GROUP, hm * GROUP), 0)
    groups = row_count // GROUP
    for h in range(hm):
        source = first_wide[h // per]
        at = (h % per) * wide
        for g in range(groups):
            rows = slice(g * GROUP, (g + 1) * GROUP)
            place = slice(h * GROUP, (h + 1) * GROUP)
            w_first[g, place, :wide] = jnp.where(
                on_diag, source[rows, at : at + wide], 0.0
            ).astype(BF16)
            bias[g, place, :] = jnp.broadcast_to(rest_bf[rows, h : h + 1].astype(F32), (GROUP, LANES))
    for o in range(outs):
        pattern = jnp.where(
            iota(second_shape, 0) == hm + (iota(second_shape, 1) // GROUP) * outs + o, 1.0, 0.0
        ).astype(BF16)
        second = jnp.dot(rest_bf, pattern, preferred_element_type=F32)
        for g in range(groups):
            w_second[g, o * GROUP : (o + 1) * GROUP, :] = jnp.where(
                on_second, second[g * GROUP : (g + 1) * GROUP], 0.0
            ).astype(BF16)

    step = LANES * math.gcd(width // LANES, 14)

    @pl.loop(0, width // step)
    def _(k):
        at = pl.ds(pl.multiple_of(k * step, LANES), step)
        col_rows = jnp.dot(pick_bf, cols_ref[:, at], preferred_element_type=F32)
        for g in range(groups):
            rows = slice(g * GROUP, (g + 1) * GROUP)
            inv = lax.rsqrt(col_rows[rows] * row_coef[rows] + EPSILON)
            grad = grads_ref[rows, at].astype(F32)
            mom = moments_ref[0, rows, at].astype(F32)
            grad_norm = grad * inv
            mom_norm = mom * inv
            parts = (
                grad_norm,
                mom_norm,
                moments_ref[1, rows, at].astype(F32) * inv,
                moments_ref[2, rows, at].astype(F32) * inv,
                grad * scale_rows[rows, 0:1],
                mom * scale_rows[rows, 1:2],
                params_ref[rows, at] * scale_rows[rows, 2:3],
                grad_norm * mom_norm,
            )
            inputs = jnp.concatenate([x.astype(BF16) for x in parts], axis=0)
            units = jnp.dot(w_first[g], inputs, preferred_element_type=F32)
            units = units + jnp.concatenate([bias[g]] * (step // LANES), axis=1)
            units = jnp.maximum(units.astype(BF16), jnp.zeros((), BF16))
            result = jnp.dot(w_second[g], units, preferred_element_type=F32)
            update_ref[rows, at] = (
                result[:GROUP]
                * jnp.exp(jnp.tanh(result[GROUP : 2 * GROUP]))
                * jax.nn.sigmoid(result[2 * GROUP :])
            )


def on_device(
    fsdp,
    rep,
    params,
    grads,
    moments,
    row_acc,
    lengths,
    tensor_order,
    col_acc,
    hidden_state,
    cell_state,
    lstm_in,
    lstm_rec,
    lstm_bias,
    hyper_first,
    hyper_rest,
):
    row_count, width = params.shape
    slots = lengths.shape[0]
    own, hid = hidden_state.shape
    hm = hyper_rest.shape[1] // 4
    fin = hyper_first.shape[1] // hm
    outs = (hyper_rest.shape[1] - hm) // hm
    groups = row_count // GROUP
    lengths = lengths.reshape(1, slots)
    order = tensor_order.reshape(1, slots)
    in_vmem = pl.BlockSpec(memory_space=pltpu.VMEM)

    anywhere = pl.BlockSpec(memory_space=pl.ANY)
    per_rep = -(-(width // LANES + 1) // rep)
    padded = rep * per_rep * LANES

    cols, gates, cell_all, row_stats = pl.pallas_call(
        functools.partial(share_kernel, fsdp, rep),
        out_shape=(
            jax.ShapeDtypeStruct((slots, padded), BF16),
            jax.ShapeDtypeStruct((slots, lstm_rec.shape[1]), F32),
            jax.ShapeDtypeStruct((slots, hid), F32),
            jax.ShapeDtypeStruct((row_count, LANES), F32),
        ),
        in_specs=[anywhere] * 4 + [in_vmem] * 6,
        out_specs=[in_vmem] * 4,
        scratch_shapes=[
            pltpu.VMEM(params.shape, params.dtype),
            pltpu.VMEM(grads.shape, grads.dtype),
            pltpu.VMEM(moments.shape, moments.dtype),
            pltpu.VMEM(lstm_rec.shape, lstm_rec.dtype),
            pltpu.VMEM((slots, padded), BF16),
            pltpu.VMEM((rep, slots, per_rep * LANES), BF16),
            pltpu.VMEM((slots, per_rep * LANES), BF16),
            pltpu.VMEM((fsdp, slots, LANES), BF16),
            pltpu.VMEM((slots, LANES), BF16),
            pltpu.VMEM((slots, padded), BF16),
            pltpu.VMEM((fsdp, own, LANES), F32),
            pltpu.VMEM((slots, LANES), F32),
            pltpu.VMEM((fsdp, own, hid), F32),
            pltpu.VMEM((slots, hid), F32),
            pltpu.VMEM((fsdp, own, hid), F32),
            pltpu.SemaphoreType.DMA((4,)),
            pltpu.SemaphoreType.DMA((7,)),
            pltpu.SemaphoreType.DMA((7,)),
            pltpu.SemaphoreType.DMA((per_rep,)),
            pltpu.SemaphoreType.DMA((per_rep,)),
        ],
        compiler_params=pltpu.CompilerParams(collective_id=0, has_side_effects=True),
        name="share",
    )(
        params,
        grads,
        moments,
        lstm_rec,
        lstm_bias.reshape(1, -1),
        lengths,
        order,
        col_acc,
        hidden_state,
        cell_state,
    )

    update, row_new, col_new, hidden_new, cell_new = pl.pallas_call(
        functools.partial(update_kernel, rep, own),
        out_shape=(
            jax.ShapeDtypeStruct((row_count, width), F32),
            jax.ShapeDtypeStruct((1, row_count), F32),
            jax.ShapeDtypeStruct((own, width), F32),
            jax.ShapeDtypeStruct((own, hid), F32),
            jax.ShapeDtypeStruct((own, hid), F32),
        ),
        in_specs=[in_vmem] * 13,
        out_specs=[in_vmem] * 5,
        scratch_shapes=[
            pltpu.VMEM((slots, width), F32),
            pltpu.VMEM((groups, hm * GROUP, fin * GROUP), BF16),
            pltpu.VMEM((groups, outs * GROUP, hm * GROUP), BF16),
            pltpu.VMEM((groups, hm * GROUP, LANES), F32),
        ],
        name="update",
    )(
        params,
        grads,
        moments,
        row_acc.reshape(1, row_count),
        lengths,
        order,
        cols,
        gates,
        cell_all,
        row_stats,
        lstm_in,
        hyper_first,
        hyper_rest,
    )
    return (update, row_new.reshape(row_count), col_new, hidden_new, cell_new)


def solution(mesh):
    rows = P(("fsdp", "rep"), None)
    flat = P(("fsdp", "rep"))
    own = P("fsdp", None)
    return jax.shard_map(
        functools.partial(on_device, mesh.shape["fsdp"], mesh.shape["rep"]),
        mesh=mesh,
        in_specs=(rows, rows, P(None, ("fsdp", "rep"), None), flat, P(), P(), own, own, own)
        + (P(),) * 5,
        out_specs=(rows, flat, own, own, own),
        check_vma=False,
    )
```
